32 devices in a mesh: row: 4 (over y, x), col: 8 (over z, core).
Axes of the slice: x: 2, y: 2, z: 4, core: 2. Of those that a mesh axis runs over, the one named last changes fastest.
Arguments:
- patches: bfloat16 [32, 128, 768], P('row', 'col'), may hold values from -6 to 6
- w_patch: bfloat16 [768, 6144], replicated, may hold values from -0.21875 to 0.21875
- patch_bias: bfloat16 [6144], replicated, may hold values from -5 to 5
- ln_gain: bfloat16 [6144], replicated, may hold values from 0.5 to 1.5
- w_qkv: bfloat16 [6144, 3, 48, 128], P(None, None, 'col'), may hold values from -1 to 1
- qk_gain: float32 [2, 48, 128], P(None, 'col'), may hold values from 0 to 6, as said below
- w_out: bfloat16 [48, 128, 6144], P('col', None, 'row'), may hold values from -0.078125 to 0.078125
Outputs:
- attn_branch: bfloat16 [4096, 6144], P(('row', 'col'))
The draws below stay inside these ranges and needn't reach their ends.
Inputs may be any that keep to these rules, and one draw needn't show every extreme that they name: `qk_gain`: positive gains.
All inputs are finite; a program needn't handle non-finite values.
Results may differ from the reference program's by a relative error of at most 0.015.
Values may be sent and summed in bfloat16 or wider, within the bound.
No kernel may reach another device: no remote copies, remote signals or barrier semaphores. Data moves between devices by JAX's collectives and lax.ppermute only.
A program may use at most 320 MiB of HBM per device.

```python
import math
import jax
import jax.numpy as jnp
from jax import lax

D = 6144
H = 48
HD = 128
PATCH_IN = 768
GW = 128
GH = 32
N_COL = 8


def draw_patches(key, part):
    key_one = jax.random.fold_in(key, 0)
    result = jnp.clip(jax.random.normal(key_one, (GH, GW, PATCH_IN), jnp.float32), -6.0, 6.0)
    return result.astype(jnp.bfloat16)


def draw_w_qkv(key, part):
    key_weight = jax.random.fold_in(key, 0)
    raw_draw = jnp.clip(jax.random.normal(key_weight, (D, 3, H, HD), jnp.float32), -6.0, 6.0) * D ** (-0.5)
    return raw_draw.astype(jnp.bfloat16)


def draw_qk_gain(key, part):
    key_head, key_dim = jax.random.split(key, 2)
    head_scale = jnp.exp(jax.random.uniform(key_head, (2, H, 1), jnp.float32, 0.5, 1.5))
    gains = head_scale * (1.0 + 0.1 * jnp.clip(jax.random.normal(key_dim, (2, H, HD), jnp.float32), -3.0, 3.0))
    return gains.astype(jnp.float32)


def shard_levels(key, extent, cuts, smallest, largest):
    def one(dim, shards_of):
        heights = jax.random.uniform(jax.random.fold_in(jax.random.fold_in(key, 6), dim), (shards_of,), jnp.float32, smallest / len(cuts), largest / len(cuts))
        return jnp.repeat(jnp.exp(heights), extent[dim] // shards_of).reshape((-1,) + (1,) * (len(extent) - dim - 1))

    gain = one(*cuts[0])
    for cut in cuts[1:]:
        gain = gain * one(*cut)
    return gain


def centred(stream_key, dims, spread, limit, pieces=(), held_as=jnp.bfloat16):
    entries = jax.random.normal(stream_key, dims, jnp.float32) * spread
    if len(pieces) > 0:
        entries = shard_levels(stream_key, dims, pieces, -0.22, 0.18) * entries
    return jnp.clip(entries, min=-limit, max=limit).astype(held_as)


def setup_inputs(seed: int = 0) -> dict:
    arg_keys = jax.random.split(jax.random.key(seed), 8)
    patches = draw_patches(jax.random.fold_in(arg_keys[7], 71), 0)
    w_patch = centred(arg_keys[1], (PATCH_IN, D), PATCH_IN ** -0.5, 0.21875)
    patch_bias = centred(arg_keys[2], (D,), 1.0, 5.0)
    ln_gain = jnp.clip(1.0 + 0.1 * jax.random.normal(arg_keys[3], (D,), jnp.float32), 0.5, 1.5).astype(jnp.bfloat16)
    w_qkv = draw_w_qkv(jax.random.fold_in(arg_keys[7], 71), 0)
    qk_gain = draw_qk_gain(jax.random.fold_in(arg_keys[7], 71), 0)
    w_out = centred(arg_keys[6], (H, HD, D), (H * HD) ** -0.5, 0.078125, ((0, 8), (2, 4)))
    return dict(patches=patches, w_patch=w_patch, patch_bias=patch_bias, ln_gain=ln_gain, w_qkv=w_qkv, qk_gain=qk_gain, w_out=w_out)


NORM_EPS = 1e-06

def sincos_table(row_ids, col_ids, model_width):
    quarter = model_width // 4
    frequency = 1.0 / 10000.0 ** (jnp.arange(quarter, dtype=jnp.float32) / quarter)
    row_angle = row_ids.astype(jnp.float32)[:, None] * frequency[None, :]
    col_angle = col_ids.astype(jnp.float32)[:, None] * frequency[None, :]
    return jnp.concatenate([jnp.sin(row_angle), jnp.cos(row_angle), jnp.sin(col_angle), jnp.cos(col_angle)], axis=1)

def layer_norm(values, gain_row):
    mean_val = lax.optimization_barrier(jnp.mean(values, axis=-1, keepdims=True))
    centered = values - mean_val
    variance = lax.optimization_barrier(jnp.mean(centered * centered, axis=-1, keepdims=True))
    return centered * lax.rsqrt(variance + NORM_EPS) * gain_row

def reference(patches, w_patch, patch_bias, ln_gain, w_qkv, qk_gain, w_out):
    token_count = GH * GW
    token_ids = jnp.arange(token_count, dtype=jnp.int32)
    flat_pixels = patches.reshape(token_count, PATCH_IN)
    embedded = jnp.dot(flat_pixels, w_patch, preferred_element_type=jnp.float32)
    embedded = embedded + patch_bias.astype(jnp.float32)[None, :] + sincos_table(token_ids // GW, token_ids % GW, D)
    normed = layer_norm(embedded, ln_gain.astype(jnp.float32)).astype(jnp.bfloat16)
    projected = jnp.dot(normed, w_qkv.reshape(D, 3 * H * HD), preferred_element_type=jnp.float32)
    projected = projected.reshape(token_count, 3, H, HD)
    queries = layer_norm(projected[:, 0], qk_gain[0]).astype(jnp.bfloat16)
    keys_all = layer_norm(projected[:, 1], qk_gain[1]).astype(jnp.bfloat16)
    values_all = projected[:, 2].astype(jnp.bfloat16)
    scale_factor = 1.0 / math.sqrt(HD)
    query_block = math.gcd(token_count, 1024)

    def one_head(head_args):
        head_q, head_k, head_v = head_args

        def one_block(block_q):
            scores = jnp.dot(block_q, head_k.T, preferred_element_type=jnp.float32) * scale_factor
            row_peak = lax.optimization_barrier(jnp.max(scores, axis=1, keepdims=True))
            exponent = jnp.exp(scores - row_peak)
            weight_sum = lax.optimization_barrier(jnp.sum(exponent, axis=1, keepdims=True))
            mixed_sum = jnp.dot(exponent.astype(jnp.bfloat16), head_v, preferred_element_type=jnp.float32)
            return (mixed_sum / weight_sum).astype(jnp.bfloat16)
        blocks = lax.map(one_block, head_q.reshape(token_count // query_block, query_block, HD))
        return blocks.reshape(token_count, HD)
    context = lax.map(one_head, (queries.transpose(1, 0, 2), keys_all.transpose(1, 0, 2), values_all.transpose(1, 0, 2)))
    context = context.transpose(1, 0, 2).reshape(token_count, H * HD)
    grouped_ctx = context.reshape(token_count, N_COL, H // N_COL * HD).transpose(1, 0, 2)
    grouped_w = w_out.reshape(N_COL, H // N_COL * HD, D)

    def add_group(running, group_args):
        group_ctx, group_w = group_args
        partial_term = jnp.dot(group_ctx, group_w, preferred_element_type=jnp.float32)
        rounded = lax.optimization_barrier(partial_term.astype(jnp.bfloat16))
        return (running + rounded.astype(jnp.float32), None)
    summed, unused = lax.scan(add_group, jnp.zeros((token_count, D), jnp.float32), (grouped_ctx, grouped_w))
    return summed.astype(jnp.bfloat16)
```

```python
import functools
import math

import jax
import jax.numpy as jnp
from jax import lax
from jax.experimental import pallas as pl
from jax.experimental.pallas import tpu as pltpu
from jax.sharding import Mesh, PartitionSpec as P

NORM_EPS = 1e-06
MIB = 1024 * 1024
NT = (((1,), (1,)), ((), ()))


def sincos_halves(ids, model_width):
    quarter = model_width // 4
    frequency = 1.0 / 10000.0 ** (jnp.arange(quarter, dtype=jnp.float32) / quarter)
    angle = ids.astype(jnp.float32)[:, None] * frequency[None, :]
    return jnp.concatenate([jnp.sin(angle), jnp.cos(angle)], axis=1)


def params(limit_mib, sem):
    return pltpu.CompilerParams(dimension_semantics=sem, vmem_limit_bytes=limit_mib * MIB)


def embed_body(px_ref, w_ref, bias_ref, gain_ref, row_ref, col_ref, out_ref, e_ref):
    rows, width, pixel = px_ref.shape
    tokens = rows * width
    model = w_ref.shape[1]
    half = model // 2
    px = px_ref[...].reshape(tokens, pixel)
    step = math.gcd(half, 1024)
    for n in range(0, model, step):
        part = jnp.dot(px, w_ref[:, n : n + step], preferred_element_type=jnp.float32)
        part = (part + bias_ref[:, n : n + step]).reshape(rows, width, step)
        if n < half:
            part = part + row_ref[:, :, n : n + step]
        else:
            part = part + col_ref[:, n - half : n - half + step][None]
        e_ref[:, n : n + step] = part.reshape(tokens, step)
    group = 16
    lanes = math.gcd(group * 4, tokens) // group

    def body(i, carry):
        for u in range(lanes):
            at = pl.ds(pl.multiple_of((i * lanes + u) * group, group), group)
            v = e_ref[at, :]
            mean = jnp.sum(v, axis=1, keepdims=True) * (1.0 / model)
            v = v - mean
            var = jnp.sum(v * v, axis=1, keepdims=True) * (1.0 / model)
            out_ref[at, :] = (v * lax.rsqrt(var + NORM_EPS) * gain_ref[...]).astype(out_ref.dtype)
        return carry

    lax.fori_loop(0, tokens // (group * lanes), body, 0)


def embed_norm(pixels, w_patch, bias_row, gain_row, row_table, col_table):
    rows, width, pixel = pixels.shape
    model = w_patch.shape[1]
    block = math.gcd(rows, max(1, 256 // width))
    once = pl.Buffered(1)
    return pl.pallas_call(
        embed_body,
        grid=(rows // block,),
        in_specs=[
            pl.BlockSpec((block, width, pixel), lambda i: (i, 0, 0)),
            pl.BlockSpec((pixel, model), lambda i: (0, 0), pipeline_mode=once),
            pl.BlockSpec((1, model), lambda i: (0, 0)),
            pl.BlockSpec((1, model), lambda i: (0, 0)),
            pl.BlockSpec((block, 1, model // 2), lambda i: (i, 0, 0)),
            pl.BlockSpec((width, model // 2), lambda i: (0, 0), pipeline_mode=once),
        ],
        out_specs=pl.BlockSpec((block * width, model), lambda i: (i, 0)),
        out_shape=jax.ShapeDtypeStruct((rows * width, model), jnp.bfloat16),
        scratch_shapes=[pltpu.VMEM((block * width, model), jnp.float32)],
        compiler_params=params(40, ("arbitrary",)),
        name="embed_norm",
    )(pixels, w_patch, bias_row, gain_row, row_table[:, None, :], col_table)


def project_body(x_ref, w_ref, *refs, norm, tile):
    gain_ref, out_ref = refs if norm else (None, refs[0])
    group, _, size = w_ref.shape
    w = jnp.concatenate([w_ref[h] for h in range(group)], axis=1)

    def body(i, carry):
        at = pl.ds(pl.multiple_of(i * tile, tile), tile)
        full = jnp.dot(x_ref[at, :], w, preferred_element_type=jnp.float32)
        for h in range(group):
            v = full[:, h * size : (h + 1) * size]
            if norm:
                v = v - jnp.mean(v, axis=1, keepdims=True)
                var = jnp.mean(v * v, axis=1, keepdims=True)
                v = v * lax.rsqrt(var + NORM_EPS) * gain_ref[h]
            out_ref[h, at, :] = v.astype(out_ref.dtype)
        return carry

    lax.fori_loop(0, x_ref.shape[0] // tile, body, 0)


def project(normed, weight, which, gain, name):
    tokens, model = normed.shape
    _, heads, _, size = weight.shape
    group = 2 if heads % 2 == 0 else heads
    norm = gain is not None
    in_specs = [
        pl.BlockSpec((tokens, model), lambda g: (0, 0), pipeline_mode=pl.Buffered(1)),
        pl.BlockSpec((None, group, model, size), lambda g: (which, g, 0, 0)),
    ]
    operands = [normed, weight]
    if norm:
        in_specs.append(pl.BlockSpec((group, 1, size), lambda g: (g, 0, 0)))
        operands.append(gain[:, None, :])
    return pl.pallas_call(
        functools.partial(project_body, norm=norm, tile=math.gcd(tokens, 512)),
        grid=(heads // group,),
        in_specs=in_specs,
        out_specs=pl.BlockSpec((group, tokens, size), lambda g: (g, 0, 0)),
        out_shape=jax.ShapeDtypeStruct((heads, tokens, size), jnp.bfloat16),
        compiler_params=params(40, ("arbitrary",)),
        name=name,
    )(*operands)


def attend_body(*refs, pairs, first, last, scale, key_block):
    q_ref, refs = refs[0], refs[1:]
    kv, refs = refs[: 2 * pairs], refs[2 * pairs :]
    if not first:
        peak_in, acc_in, refs = refs[0], refs[1], refs[2:]
    size = q_ref.shape[-1]
    rows = math.prod(q_ref.shape[:-1])
    q = q_ref[...].reshape(rows, size)
    ones = jnp.ones((key_block, size), jnp.bfloat16)
    blocks = []
    for c in range(pairs):
        for b in range(kv[2 * c].shape[0] // key_block):
            blocks.append((kv[2 * c], kv[2 * c + 1], b * key_block))

    def score(i):
        k_ref, _, at = blocks[i]
        return lax.dot_general(q, k_ref[at : at + key_block, :], NT, preferred_element_type=jnp.float32)

    if first:
        peak = None
        acc = None
    else:
        peak = peak_in[...].reshape(rows, size)[:, :1]
        acc = acc_in[...].reshape(rows, 2 * size)
    ahead = score(0)
    for i in range(len(blocks)):
        scores = ahead
        if i + 1 < len(blocks):
            ahead = score(i + 1)
        top = jnp.max(scores, axis=1, keepdims=True)
        new_peak = top if peak is None else jnp.maximum(peak, top)
        weights = jnp.exp2((scores - new_peak) * scale).astype(jnp.bfloat16)
        _, v_ref, at = blocks[i]
        v = jnp.concatenate([v_ref[at : at + key_block, :], ones], axis=1)
        mixed = jnp.dot(weights, v, preferred_element_type=jnp.float32)
        if peak is None:
            acc = mixed
        else:
            acc = acc * jnp.exp2((peak - new_peak) * scale) + mixed
        peak = new_peak
    if last:
        out_ref = refs[0]
        out_ref[...] = (acc[:, :size] / acc[:, size:]).astype(out_ref.dtype).reshape(out_ref.shape)
    else:
        refs[0][...] = jnp.broadcast_to(peak, (rows, size)).reshape(refs[0].shape)
        refs[1][...] = acc.reshape(refs[1].shape)


def attend(queries, kvs, state, pieces, part, parts, last, name):
    heads, tokens, size = queries.shape
    scale = math.log2(math.e) / math.sqrt(size)
    keys = kvs[0][0].shape[1]
    key_block = math.gcd(keys, 1024)
    run = tokens // pieces
    cut = run // parts
    if part is None:
        qb = math.gcd(tokens, 512)
        grid = (heads, tokens // qb)
        view = lambda a: a
        block = lambda width: pl.BlockSpec((None, qb, width), lambda h, i: (h, i, 0))
        out_rows = tokens
    else:
        grid = (heads, 1)
        qb = pieces * cut
        view = lambda a: a.reshape(heads, pieces, parts, cut, a.shape[-1])
        block = lambda width: pl.BlockSpec((None, pieces, None, cut, width), lambda h, i: (h, 0, part, 0, 0))
        out_rows = pieces * cut
    whole = pl.BlockSpec((None, keys, size), lambda h, i: (h, 0, 0))
    operands = [view(queries)]
    in_specs = [block(size)]
    for k, v in kvs:
        operands += [k, v]
        in_specs += [whole, whole]
    if state is not None:
        operands += [view(state[0]), view(state[1])]
        in_specs += [block(size), block(2 * size)]
    if last:
        out_specs = pl.BlockSpec((qb, size), lambda h, i: (i, h))
        out_shape = jax.ShapeDtypeStruct((out_rows, heads * size), jnp.bfloat16)
    else:
        out_specs = [block(size), block(2 * size)]
        out_shape = [
            jax.ShapeDtypeStruct((heads, tokens, size), jnp.float32),
            jax.ShapeDtypeStruct((heads, tokens, 2 * size), jnp.float32),
        ]
    return pl.pallas_call(
        functools.partial(
            attend_body, pairs=len(kvs), first=state is None, last=last, scale=scale, key_block=key_block
        ),
        grid=grid,
        in_specs=in_specs,
        out_specs=out_specs,
        out_shape=out_shape,
        compiler_params=params(40, ("arbitrary", "arbitrary")),
        name=name,
    )(*operands)


def swap(n, shift):
    return [(i, (i + shift) % n) for i in range(n)]


def local(patches, w_patch, patch_bias, ln_gain, w_qkv, qk_gain, w_out):
    tile_rows, tile_cols, pixel_width = patches.shape
    model = w_patch.shape[1]
    heads, size = w_qkv.shape[2], w_qkv.shape[3]
    ny, nx, nz, nc = (lax.axis_size(a) for a in ("y", "x", "z", "c"))
    row = lax.axis_index("y") * nx + lax.axis_index("x")
    z_at, c_at = lax.axis_index("z"), lax.axis_index("c")
    width = tile_cols * nz * nc

    out_weight = lax.all_gather(w_out, ("y", "x"), axis=2, tiled=True).reshape(heads * size, model)

    pieces = [patches] + [lax.ppermute(patches, "z", swap(nz, s)) for s in range(1, nz)]
    mine = jnp.stack(pieces)
    both = jnp.stack([mine, lax.ppermute(mine, "c", swap(nc, 1))])
    order_z = (z_at - jnp.arange(nz)) % nz
    order_c = (c_at - jnp.arange(nc)) % nc
    both = jnp.take(jnp.take(both, order_c, axis=0), order_z, axis=1)
    pixels = both.transpose(2, 1, 0, 3, 4).reshape(tile_rows, width, pixel_width)

    row_table = sincos_halves(row * tile_rows + jnp.arange(tile_rows, dtype=jnp.int32), model)
    col_table = sincos_halves(jnp.arange(width, dtype=jnp.int32), model)
    normed = embed_norm(
        pixels,
        w_patch,
        patch_bias.astype(jnp.float32)[None, :],
        ln_gain.astype(jnp.float32)[None, :],
        row_table,
        col_table,
    )
    weight = w_qkv.transpose(1, 2, 0, 3)
    keys = project(normed, weight, 1, qk_gain[1], "project_k")
    values = project(normed, weight, 2, None, "project_v")
    queries = project(normed, weight, 0, qk_gain[0], "project_q")

    flip = swap(nx, 1)
    keys_x = lax.ppermute(keys, "x", flip)
    keys_y = [lax.ppermute(keys, "y", swap(ny, s)) for s in range(1, ny)]
    values_x = lax.ppermute(values, "x", flip)
    values_y = [lax.ppermute(values, "y", swap(ny, s)) for s in range(1, ny)]
    keys_far = [lax.ppermute(keys_x, "y", swap(ny, s)) for s in range(1, ny)]
    values_far = [lax.ppermute(v, "x", flip) for v in values_y]

    runs = nz * nc
    state = attend(queries, [(keys, values)], None, runs, None, 1, False, "attend_own")
    near = [(keys_x, values_x)] + list(zip(keys_y, values_y))
    state = attend(queries, near, state, runs, None, 1, False, "attend_near")
    far = list(zip(keys_far, values_far))
    parts = 2
    outs = []
    for part in range(parts):
        context = attend(queries, far, state, runs, part, parts, True, "attend_far")
        partial = jnp.dot(context, out_weight, preferred_element_type=jnp.float32).astype(jnp.bfloat16)
        outs.append(lax.psum_scatter(partial, ("z", "c"), scatter_dimension=0, tiled=True))
    return jnp.concatenate(outs, axis=0)


def solution(mesh):
    rows, cols = mesh.shape["row"], mesh.shape["col"]
    fine = Mesh(mesh.devices.reshape(rows // 2, 2, cols // 2, 2), ("y", "x", "z", "c"))
    row, col = ("y", "x"), ("z", "c")
    return jax.shard_map(
        local,
        mesh=fine,
        in_specs=(
            P(row, col, None),
            P(),
            P(),
            P(),
            P(None, None, col, None),
            P(None, col, None),
            P(col, None, row),
        ),
        out_specs=P((*row, *col), None),
        check_vma=False,
    )
```
